32 devices in a mesh: blk: 8 (over z, x), grp: 4 (over y, core).
Axes of the slice: x: 2, y: 2, z: 4, core: 2. Of those that a mesh axis runs over, the one named last changes fastest.
Arguments:
- amplitudes: bfloat16 [8, 512, 1024], P('blk', None, 'grp'), may hold values from -6 to 6
- integrals: bfloat16 [64, 1024, 1024], P('blk', 'grp'), may hold values from -0.1875 to 0.1875
- cd_index: int32 [64], replicated, may hold values from 0 to 7, as said below
- live_blocks: int32 [8], replicated, may hold values from 4 to 8, as said below
- occ_energy: float32 [512], P('grp'), may hold values from -3 to -0.5
- vir_energy: float32 [8, 1024], P('blk'), may hold values from 0.5 to 4
Outputs:
- amplitude_step: float32 [8, 512, 1024], P('blk', 'grp')
The draws below stay inside these ranges and needn't reach their ends.
Inputs may be any that keep to these rules, and one draw needn't show every extreme that they name: (cd_index[k] - k // 8) mod 8 is at most 2 or at least 6; among the first 4 slots of each pair block every nonzero offset from -2 to 2 occurs once. `live_blocks`: 8 is reached by some pair block in every draw.
All inputs are finite; a program needn't handle non-finite values.
Results may differ from the reference program's by a relative error of at most 0.0003.
Values may be sent and summed in bfloat16 or wider, within the bound.
A program may use at most 64 MiB of HBM per device.

```python
import jax
import jax.numpy as jnp
from jax import lax

PW = 1024
OCC = 512
INT_DEV = 8
REACH = 2
NPB = 8
NINT = 64


def draw_cd_index(key, part):
    key_list = jax.random.split(jax.random.fold_in(key, 11), 2)
    shifts = jax.random.randint(key_list[0], (NPB, INT_DEV), -REACH, REACH + 1).astype(jnp.int32)
    rotation = jax.random.randint(key_list[1], (NPB, 1), 0, 2 * REACH).astype(jnp.int32)
    slot_ids = jnp.arange(INT_DEV, dtype=jnp.int32)[None, :]
    cycled = jnp.mod(slot_ids + rotation, 2 * REACH)
    covered = cycled - REACH + (cycled >= REACH).astype(jnp.int32)
    shifts = jnp.where(slot_ids < 2 * REACH, covered, shifts)
    owners = jnp.arange(NPB, dtype=jnp.int32)[:, None]
    return jnp.mod(owners + shifts, NPB).reshape(NINT).astype(jnp.int32)


def draw_live_blocks(key, part):
    key_list = jax.random.split(jax.random.fold_in(key, 23), 3)
    base_live = jax.random.randint(key_list[0], (NPB,), 2 * REACH, 2 * REACH + 2)
    base_live = jnp.minimum(base_live, INT_DEV)
    heavy_rows = jax.random.randint(key_list[1], (NPB,), 0, 8) == 0
    live_counts = jnp.where(heavy_rows, INT_DEV, base_live)
    full_row = jax.random.randint(key_list[2], (), 0, NPB)
    return live_counts.at[full_row].set(INT_DEV).astype(jnp.int32)


def block_levels(stream_key, extent, pieces, least, top_value):
    def one(axis_at, blocks):
        heights = jax.random.uniform(jax.random.fold_in(jax.random.fold_in(stream_key, 6), axis_at), (blocks,), jnp.float32, least / len(pieces), top_value / len(pieces))
        return jnp.repeat(jnp.exp(heights), extent[axis_at] // blocks).reshape((-1,) + (1,) * (len(extent) - axis_at - 1))

    factor_of = one(*pieces[0])
    for cut in pieces[1:]:
        factor_of = factor_of * one(*cut)
    return factor_of


def bell_draw(own_key, extent, width, bound, cuts=(), held_as=jnp.bfloat16):
    array = jax.random.normal(own_key, extent, jnp.float32) * width
    if len(cuts) > 0:
        array = block_levels(own_key, extent, cuts, -0.22, 0.18) * array
    return jnp.clip(array, min=-bound, max=bound).astype(held_as)


def setup_inputs(seed: int = 0) -> dict:
    keys = jax.random.split(jax.random.key(seed), 7)
    return {
        "amplitudes": bell_draw(keys[0], (NPB, OCC, PW), 1.0, 6.0, ((0, 8), (2, 4))),
        "integrals": bell_draw(keys[1], (NINT, PW, PW), PW ** -0.5, 0.1875, ((0, 8), (1, 4))),
        "cd_index": draw_cd_index(jax.random.fold_in(keys[6], 71), 0),
        "live_blocks": draw_live_blocks(jax.random.fold_in(keys[6], 71), 0),
        "occ_energy": jnp.clip(-3.0 + 2.5 * jax.random.uniform(keys[4], (OCC,), jnp.float32) ** block_levels(keys[4], (OCC,), ((0, 4),), -0.2, 0.2), -3.0, -0.5),
        "vir_energy": jnp.clip(0.5 + 3.5 * jax.random.uniform(keys[5], (NPB, PW), jnp.float32) ** block_levels(keys[5], (NPB, PW), ((0, 8),), -0.2, 0.2), 0.5, 4.0),
    }


def reference(amplitudes, integrals, cd_index, live_blocks, occ_energy, vir_energy):
    def one_block(block_index):
        def add_task(running, slot_index):
            task_index = block_index * INT_DEV + slot_index

            def product(running):
                amp_block = amplitudes[cd_index[task_index]]
                return running + jnp.dot(amp_block, integrals[task_index], preferred_element_type=jnp.float32)

            def unchanged(running):
                return running

            return lax.cond(slot_index < live_blocks[block_index], product, unchanged, running), None

        start_sum = jnp.zeros((OCC, PW), jnp.float32)
        ladder, _ = lax.scan(add_task, start_sum, jnp.arange(INT_DEV, dtype=jnp.int32))
        denominator = vir_energy[block_index][None, :] - occ_energy[:, None]
        return ladder / denominator

    return lax.map(one_block, jnp.arange(NPB, dtype=jnp.int32))
```

```python
import functools

import jax
import jax.numpy as jnp
from jax import lax
from jax.experimental import pallas as pl
from jax.experimental.pallas import tpu as pltpu
from jax.sharding import PartitionSpec as P

REACH = 2
FAR = (4, 4, 4, 4)
NEAR = (4, 4, 4, 4)
LEAD = 3
AHEAD = 5
LOOK = 2
TILE = 512
MESH = pl.DeviceIdType.MESH
COMPUTE, MATE, YEX, AMP = True, True, True, True
LANES = 128
TOP = 32760.0


def plan(rows, groups):
    owned = rows // groups
    hops = groups // 2
    far = [owned * p // sum(FAR) for p in FAR]
    near = [owned * p // sum(NEAR) for p in NEAR]
    out = []
    for hop in range(1, hops + 1):
        at = 0
        for piece in (far if hop < hops else near):
            out.append((hop % hops, at, piece))
            at += piece
    return out


def ladder_kernel(blocks, groups, cd_ref, live_ref, amp_ref, int_ref, out_ref, *scratch):
    slots, depth, cols = int_ref.shape
    rows = amp_ref.shape[1]
    halves = groups // 2
    owned = rows // groups
    chunks = plan(rows, groups)
    steps = len(chunks)
    far_steps = sum(1 for c in chunks if c[0])
    window = 2 * REACH + 1
    near, own, pair_out, pair_in = (scratch[i * steps:(i + 1) * steps] for i in range(4))
    rest = scratch[4 * steps:]
    far_out, far_in = rest[:far_steps], rest[far_steps:2 * far_steps]
    (cd_smem, live_smem, table_sem, weights, peak_out, peak_in, amp_sem, int_sem, amp_send, amp_recv,
     pair_send, pair_recv, far_send, far_recv) = rest[2 * far_steps:]

    here = lax.axis_index("blk")
    me = lax.axis_index("grp")
    half, core = me // 2, me % 2
    mate = half * 2 + 1 - core
    side = 1 - 2 * (here % 2)
    twin = here + side
    ahead, behind = (here + 2 * side + blocks) % blocks, (here - 2 * side + blocks) % blocks

    amp_loads = []
    for step, (hop, at, piece) in enumerate(chunks):
        there = (half + hop) % halves
        for part, lane in enumerate((1 - core, core)):
            start = pl.multiple_of((there * 2 + lane) * owned + at, 16)
            amp_loads.append(pltpu.make_async_copy(
                amp_ref.at[0, pl.ds(start, piece)],
                near[step].at[REACH, pl.ds(part * piece, piece)],
                amp_sem.at[step, part]))
    int_loads = [pltpu.make_async_copy(int_ref.at[k], weights.at[pl.ds(k * depth, depth)], int_sem.at[k])
                 for k in range(slots)]
    table_loads = [pltpu.make_async_copy(cd_ref, cd_smem, table_sem.at[0]),
                   pltpu.make_async_copy(live_ref, live_smem, table_sem.at[1])]
    for load in amp_loads:
        load.start()

    barrier = pltpu.get_barrier_semaphore()
    for target in (ahead, behind, twin):
        pl.semaphore_signal(barrier, inc=1, device_id={"blk": target}, device_id_type=MESH)
    pl.semaphore_signal(barrier, inc=1, device_id={"grp": mate}, device_id_type=MESH)
    for hop in range(1, halves):
        pl.semaphore_signal(barrier, inc=1, device_id={"grp": (half + hop) % halves * 2 + core}, device_id_type=MESH)
    for load in table_loads:
        load.start()
    pl.semaphore_wait(barrier, 3 + halves)

    def push(step, source, slot, lane, target):
        return pltpu.make_async_remote_copy(
            near[step].at[source], near[step].at[slot], amp_send.at[lane, step], amp_recv.at[slot, step],
            device_id={"blk": target}, device_id_type=MESH)

    def arrival(step, slot):
        if AMP:
            push(step, REACH, slot, 0, twin).wait_recv()

    sent = []

    def launch(copy):
        if AMP:
            copy.start()
            sent.append(copy)

    def push_passed(step):
        if step < steps:
            launch(push(step, REACH, REACH + 2 * side, 0, behind))

    def push_kept(step):
        if 0 <= step < steps:
            launch(push(step, REACH, REACH - 2 * side, 1, ahead))

    def push_twin(step):
        if step < steps:
            launch(push(step, REACH, REACH - side, 2, twin))

    def forward(step):
        if step < steps:
            arrival(step, REACH + 2 * side)
            launch(push(step, REACH + 2 * side, REACH + side, 3, twin))
            push_twin(step + AHEAD)

    for step in range(steps + LEAD):
        if step < steps:
            amp_loads[2 * step].wait()
            amp_loads[2 * step + 1].wait()
            push_passed(step)
            if step < AHEAD:
                push_twin(step)
        push_kept(step - LEAD)
    for load in int_loads:
        load.start()
    for step in range(steps):
        near[step][window] = jnp.zeros(near[step].shape[1:], near[step].dtype)

    for load in table_loads:
        load.wait()
    picks = []
    for k in range(slots):
        offset = (cd_smem[here * slots + k] - here + REACH + blocks) % blocks
        picks.append(jnp.where(k < live_smem[here], offset, window))

    pair_copies, far_copies = [], []

    def settle(step):
        hop, at, piece = chunks[step]
        if MATE:
            pair_copies[step].wait_recv()
        total = own[step][...] + pair_in[step][...]
        if hop:
            tiles = [total[:, j:j + LANES].reshape(piece // 8, 8, LANES) for j in range(0, cols, LANES)]
            peak = functools.reduce(jnp.maximum, [jnp.max(jnp.abs(t), axis=0) for t in tiles])
            peak = jnp.maximum(peak, 1e-30)
            peak_out[step] = peak * (1 / TOP)
            for j, t in enumerate(tiles):
                code = jnp.round(t * (TOP / peak)[None]).astype(jnp.int32).astype(jnp.int16)
                far_out[step][:, j * LANES:(j + 1) * LANES] = code.reshape(piece, LANES)
            there = (half + hop) % halves * 2 + core
            pair = [pltpu.make_async_remote_copy(
                source, target, far_send.at[kind, step], far_recv.at[kind, step],
                device_id={"grp": there}, device_id_type=MESH)
                for kind, (source, target) in enumerate(((far_out[step], far_in[step]), (peak_out.at[step], peak_in.at[step])))]
            if YEX:
                for copy in pair:
                    copy.start()
                far_copies.append(pair)
        else:
            out_ref[pl.ds(at, piece)] = total

    for step in range(LOOK):
        forward(step)
    for load in int_loads:
        load.wait()
    for step in range(steps):
        piece = chunks[step][2]
        forward(step + LOOK)
        for slot in (REACH - 2 * side, REACH + side, REACH - side):
            arrival(step, slot)
        if COMPUTE:
            lhs = jnp.concatenate([near[step][pick] for pick in picks], axis=1)

            @pl.loop(0, cols // TILE)
            def _(tile):
                lanes = pl.ds(pl.multiple_of(tile * TILE, TILE), TILE)
                product = jnp.dot(lhs, weights[:, lanes], preferred_element_type=jnp.float32)
                pair_out[step][:, lanes] = product[:piece]
                own[step][:, lanes] = product[piece:]

        copy = pltpu.make_async_remote_copy(
            pair_out[step], pair_in[step], pair_send.at[step], pair_recv.at[step],
            device_id={"grp": mate}, device_id_type=MESH)
        if MATE:
            copy.start()
            pair_copies.append(copy)
        if step >= 1:
            settle(step - 1)
    settle(steps - 1)
    if YEX:
        for step in range(far_steps):
            hop, at, piece = chunks[step]
            for copy in far_copies[step]:
                copy.wait_recv()
            peak = peak_in[step][None]
            for j in range(0, cols, LANES):
                code = far_in[step][:, j:j + LANES].astype(jnp.int32).astype(jnp.float32)
                value = (code.reshape(piece // 8, 8, LANES) * peak).reshape(piece, LANES)
                out_ref[pl.ds(at, piece), j:j + LANES] = out_ref[pl.ds(at, piece), j:j + LANES] + value
    for copy in sent + pair_copies + [copy for pair in far_copies for copy in pair]:
        copy.wait_send()


def body(blocks, groups, amplitudes, integrals, cd_index, live_blocks, occ_energy, vir_energy):
    slots, depth, cols = integrals.shape
    rows = amplitudes.shape[1]
    owned = rows // groups
    chunks = plan(rows, groups)
    steps = len(chunks)
    far = [c for c in chunks if c[0]]
    window = 2 * REACH + 1
    f32 = [pltpu.VMEM((c[2], cols), jnp.float32) for c in chunks]
    i16 = [pltpu.VMEM((c[2], cols), jnp.int16) for c in far]
    ladder = pl.pallas_call(
        functools.partial(ladder_kernel, blocks, groups),
        out_shape=jax.ShapeDtypeStruct((owned, cols), jnp.float32),
        in_specs=[pl.BlockSpec(memory_space=pltpu.HBM)] * 4,
        out_specs=pl.BlockSpec(memory_space=pltpu.VMEM),
        scratch_shapes=[pltpu.VMEM((window + 1, 2 * c[2], depth), amplitudes.dtype) for c in chunks] + f32 * 3 + i16 * 2 + [
            pltpu.SMEM(cd_index.shape, cd_index.dtype),
            pltpu.SMEM(live_blocks.shape, live_blocks.dtype),
            pltpu.SemaphoreType.DMA((2,)),
            pltpu.VMEM((slots * depth, cols), integrals.dtype),
            pltpu.VMEM((len(far), 8, LANES), jnp.float32),
            pltpu.VMEM((len(far), 8, LANES), jnp.float32),
            pltpu.SemaphoreType.DMA((steps, 2)),
            pltpu.SemaphoreType.DMA((slots,)),
            pltpu.SemaphoreType.DMA((4, steps)),
            pltpu.SemaphoreType.DMA((window, steps)),
            pltpu.SemaphoreType.DMA((steps,)),
            pltpu.SemaphoreType.DMA((steps,)),
            pltpu.SemaphoreType.DMA((2, len(far))),
            pltpu.SemaphoreType.DMA((2, len(far))),
        ],
        compiler_params=pltpu.CompilerParams(
            collective_id=0, has_side_effects=True, vmem_limit_bytes=24 * 1024 * 1024),
    )(*[pltpu.with_memory_space_constraint(x, pltpu.HBM) for x in (cd_index, live_blocks, amplitudes, integrals)])
    denominator = vir_energy[0][None, :] - occ_energy[:, None]
    return (ladder / denominator)[None]


def solution(mesh):
    return jax.shard_map(
        functools.partial(body, mesh.shape["blk"], mesh.shape["grp"]),
        mesh=mesh,
        in_specs=(P("blk", None, "grp"), P("blk", "grp", None), P(), P(), P("grp"), P("blk", None)),
        out_specs=P("blk", "grp", None),
        check_vma=False,
    )
```

```python
import functools

import jax
import jax.numpy as jnp
from jax import lax
from jax.experimental import pallas as pl
from jax.experimental.pallas import tpu as pltpu
from jax.sharding import PartitionSpec as P

REACH = 2
FAR = (4, 4, 4, 4)
NEAR = (4, 4, 4, 4)
LEAD = 4
AHEAD = 4
LOOK = 3
MESH = pl.DeviceIdType.MESH
LANES = 128
TOP = 32760.0


def plan(rows, groups):
    owned = rows // groups
    hops = groups // 2
    far = [owned * p // sum(FAR) for p in FAR]
    near = [owned * p // sum(NEAR) for p in NEAR]
    out = []
    for hop in range(1, hops + 1):
        at = 0
        for piece in (far if hop < hops else near):
            out.append((hop % hops, at, piece))
            at += piece
    return out


def ladder_kernel(blocks, groups, cd_ref, live_ref, amp_ref, int_ref, out_ref, *scratch):
    slots, depth, cols = int_ref.shape
    rows = amp_ref.shape[1]
    halves = groups // 2
    owned = rows // groups
    chunks = plan(rows, groups)
    steps = len(chunks)
    far_steps = sum(1 for c in chunks if c[0])
    window = 2 * REACH + 1
    near, own, pair_out, pair_in = (scratch[i * steps:(i + 1) * steps] for i in range(4))
    rest = scratch[4 * steps:]
    far_out, far_in = rest[:far_steps], rest[far_steps:2 * far_steps]
    (cd_smem, live_smem, table_sem, weights, peak_out, peak_in, amp_sem, int_sem, amp_send, amp_recv,
     pair_send, pair_recv, far_send, far_recv) = rest[2 * far_steps:]

    here = lax.axis_index("blk")
    me = lax.axis_index("grp")
    half, core = me // 2, me % 2
    mate = half * 2 + 1 - core
    side = 1 - 2 * (here % 2)
    twin = here + side
    ahead, behind = (here + 2 * side + blocks) % blocks, (here - 2 * side + blocks) % blocks

    amp_loads = []
    for step, (hop, at, piece) in enumerate(chunks):
        there = (half + hop) % halves
        for part, lane in enumerate((1 - core, core)):
            start = pl.multiple_of((there * 2 + lane) * owned + at, 16)
            amp_loads.append(pltpu.make_async_copy(
                amp_ref.at[0, pl.ds(start, piece)],
                near[step].at[REACH, pl.ds(part * piece, piece)],
                amp_sem.at[step, part]))
    int_loads = [pltpu.make_async_copy(int_ref.at[k], weights.at[pl.ds(k * depth, depth)], int_sem.at[k])
                 for k in range(slots)]
    table_loads = [pltpu.make_async_copy(cd_ref, cd_smem, table_sem.at[0]),
                   pltpu.make_async_copy(live_ref, live_smem, table_sem.at[1])]
    for load in amp_loads:
        load.start()

    barrier = pltpu.get_barrier_semaphore()
    for target in (ahead, behind, twin):
        pl.semaphore_signal(barrier, inc=1, device_id={"blk": target}, device_id_type=MESH)
    pl.semaphore_signal(barrier, inc=1, device_id={"grp": mate}, device_id_type=MESH)
    for hop in range(1, halves):
        pl.semaphore_signal(barrier, inc=1, device_id={"grp": (half + hop) % halves * 2 + core}, device_id_type=MESH)
    for load in table_loads:
        load.start()
    for step in range(steps):
        near[step][window] = jnp.zeros(near[step].shape[1:], near[step].dtype)
    pl.semaphore_wait(barrier, 3 + halves)

    def push(step, source, slot, lane, target):
        return pltpu.make_async_remote_copy(
            near[step].at[source], near[step].at[slot], amp_send.at[lane, step], amp_recv.at[slot, step],
            device_id={"blk": target}, device_id_type=MESH)

    def arrival(step, slot):
        push(step, REACH, slot, 0, twin).wait_recv()

    sent = []

    def launch(copy):
        copy.start()
        sent.append(copy)

    def push_passed(step):
        if step < steps:
            launch(push(step, REACH, REACH + 2 * side, 0, behind))

    def push_kept(step):
        if 0 <= step < steps:
            launch(push(step, REACH, REACH - 2 * side, 1, ahead))

    def push_twin(step):
        if step < steps:
            launch(push(step, REACH, REACH - side, 2, twin))

    def forward(step):
        if step < steps:
            arrival(step, REACH + 2 * side)
            launch(push(step, REACH + 2 * side, REACH + side, 3, twin))
            push_twin(step + AHEAD)

    for step in range(steps + LEAD):
        if step < steps:
            amp_loads[2 * step].wait()
            amp_loads[2 * step + 1].wait()
            push_passed(step)
            if step < AHEAD:
                push_twin(step)
        push_kept(step - LEAD)
    for load in int_loads:
        load.start()

    for load in table_loads:
        load.wait()
    picks = []
    for k in range(slots):
        offset = (cd_smem[here * slots + k] - here + REACH + blocks) % blocks
        picks.append(jnp.where(k < live_smem[here], offset, window))

    pair_copies, far_copies = [], []

    def settle(step):
        hop, at, piece = chunks[step]
        pair_copies[step].wait_recv()
        total = own[step][...] + pair_in[step][...]
        if hop:
            tiles = [total[:, j:j + LANES].reshape(piece // 8, 8, LANES) for j in range(0, cols, LANES)]
            peak = functools.reduce(jnp.maximum, [jnp.max(jnp.abs(t), axis=0) for t in tiles])
            peak = jnp.maximum(peak, 1e-30)
            peak_out[step] = peak * (1 / TOP)
            for j, t in enumerate(tiles):
                code = jnp.round(t * (TOP / peak)[None]).astype(jnp.int32).astype(jnp.int16)
                far_out[step][:, j * LANES:(j + 1) * LANES] = code.reshape(piece, LANES)
            there = (half + hop) % halves * 2 + core
            pair = [pltpu.make_async_remote_copy(
                source, target, far_send.at[kind, step], far_recv.at[kind, step],
                device_id={"grp": there}, device_id_type=MESH)
                for kind, (source, target) in enumerate(((far_out[step], far_in[step]), (peak_out.at[step], peak_in.at[step])))]
            for copy in pair:
                copy.start()
            far_copies.append(pair)
        else:
            out_ref[pl.ds(at, piece)] = total

    for step in range(LOOK):
        forward(step)
    for load in int_loads:
        load.wait()
    for step in range(steps):
        piece = chunks[step][2]
        forward(step + LOOK)
        for slot in (REACH - 2 * side, REACH + side, REACH - side):
            arrival(step, slot)
        lhs = jnp.concatenate([near[step][pick] for pick in picks], axis=1)

        product = jnp.dot(lhs, weights[...], preferred_element_type=jnp.float32)
        pair_out[step][...] = product[:piece]
        own[step][...] = product[piece:]

        copy = pltpu.make_async_remote_copy(
            pair_out[step], pair_in[step], pair_send.at[step], pair_recv.at[step],
            device_id={"grp": mate}, device_id_type=MESH)
        copy.start()
        pair_copies.append(copy)
        if step >= 1:
            settle(step - 1)
    settle(steps - 1)
    for step in range(far_steps):
        hop, at, piece = chunks[step]
        for copy in far_copies[step]:
            copy.wait_recv()
        peak = peak_in[step][None]
        for j in range(0, cols, LANES):
            code = far_in[step][:, j:j + LANES].astype(jnp.int32).astype(jnp.float32)
            value = (code.reshape(piece // 8, 8, LANES) * peak).reshape(piece, LANES)
            out_ref[pl.ds(at, piece), j:j + LANES] = out_ref[pl.ds(at, piece), j:j + LANES] + value
    for copy in sent + pair_copies + [copy for pair in far_copies for copy in pair]:
        copy.wait_send()


def body(blocks, groups, amplitudes, integrals, cd_index, live_blocks, occ_energy, vir_energy):
    slots, depth, cols = integrals.shape
    rows = amplitudes.shape[1]
    owned = rows // groups
    chunks = plan(rows, groups)
    steps = len(chunks)
    far = [c for c in chunks if c[0]]
    window = 2 * REACH + 1
    f32 = [pltpu.VMEM((c[2], cols), jnp.float32) for c in chunks]
    i16 = [pltpu.VMEM((c[2], cols), jnp.int16) for c in far]
    ladder = pl.pallas_call(
        functools.partial(ladder_kernel, blocks, groups),
        out_shape=jax.ShapeDtypeStruct((owned, cols), jnp.float32),
        in_specs=[pl.BlockSpec(memory_space=pltpu.HBM)] * 4,
        out_specs=pl.BlockSpec(memory_space=pltpu.VMEM),
        scratch_shapes=[pltpu.VMEM((window + 1, 2 * c[2], depth), amplitudes.dtype) for c in chunks] + f32 * 3 + i16 * 2 + [
            pltpu.SMEM(cd_index.shape, cd_index.dtype),
            pltpu.SMEM(live_blocks.shape, live_blocks.dtype),
            pltpu.SemaphoreType.DMA((2,)),
            pltpu.VMEM((slots * depth, cols), integrals.dtype),
            pltpu.VMEM((len(far), 8, LANES), jnp.float32),
            pltpu.VMEM((len(far), 8, LANES), jnp.float32),
            pltpu.SemaphoreType.DMA((steps, 2)),
            pltpu.SemaphoreType.DMA((slots,)),
            pltpu.SemaphoreType.DMA((4, steps)),
            pltpu.SemaphoreType.DMA((window, steps)),
            pltpu.SemaphoreType.DMA((steps,)),
            pltpu.SemaphoreType.DMA((steps,)),
            pltpu.SemaphoreType.DMA((2, len(far))),
            pltpu.SemaphoreType.DMA((2, len(far))),
        ],
        compiler_params=pltpu.CompilerParams(
            collective_id=0, has_side_effects=True, vmem_limit_bytes=24 * 1024 * 1024),
    )(*[pltpu.with_memory_space_constraint(x, pltpu.HBM) for x in (cd_index, live_blocks, amplitudes, integrals)])
    denominator = vir_energy[0][None, :] - occ_energy[:, None]
    return (ladder / denominator)[None]


def solution(mesh):
    return jax.shard_map(
        functools.partial(body, mesh.shape["blk"], mesh.shape["grp"]),
        mesh=mesh,
        in_specs=(P("blk", None, "grp"), P("blk", "grp", None), P(), P(), P("grp"), P("blk", None)),
        out_specs=P("blk", "grp", None),
        check_vma=False,
    )
```

```python
import functools

import jax
import jax.numpy as jnp
from jax import lax
from jax.experimental import pallas as pl
from jax.experimental.pallas import tpu as pltpu
from jax.sharding import PartitionSpec as P

REACH = 2
FAR = (4, 4, 4, 4)
NEAR = (4, 4, 4, 4)
LEAD = 3
AHEAD = 4
LOOK = 3
PACE = 1
MESH = pl.DeviceIdType.MESH
LANES = 128
TOP = 32760.0


def plan(rows, groups):
    owned = rows // groups
    hops = groups // 2
    far = [owned * p // sum(FAR) for p in FAR]
    near = [owned * p // sum(NEAR) for p in NEAR]
    out = []
    for hop in range(1, hops + 1):
        at = 0
        for piece in (far if hop < hops else near):
            out.append((hop % hops, at, piece))
            at += piece
    return out


def ladder_kernel(blocks, groups, cd_ref, live_ref, amp_ref, int_ref, out_ref, *scratch):
    slots, depth, cols = int_ref.shape
    rows = amp_ref.shape[1]
    halves = groups // 2
    owned = rows // groups
    chunks = plan(rows, groups)
    steps = len(chunks)
    far_steps = sum(1 for c in chunks if c[0])
    window = 2 * REACH + 1
    near, own, pair_out, pair_in = (scratch[i * steps:(i + 1) * steps] for i in range(4))
    rest = scratch[4 * steps:]
    far_out, far_in = rest[:far_steps], rest[far_steps:2 * far_steps]
    (cd_smem, live_smem, table_sem, weights, peak_out, peak_in, amp_sem, int_sem, amp_send, amp_recv,
     pair_send, pair_recv, far_send, far_recv) = rest[2 * far_steps:]

    here = lax.axis_index("blk")
    me = lax.axis_index("grp")
    half, core = me // 2, me % 2
    mate = half * 2 + 1 - core
    side = 1 - 2 * (here % 2)
    twin = here + side
    ahead, behind = (here + 2 * side + blocks) % blocks, (here - 2 * side + blocks) % blocks

    low, high = here < 2, here + 2 >= blocks
    paced = ~low & ~high

    amp_loads = []
    for step, (hop, at, piece) in enumerate(chunks):
        there = (half + hop) % halves
        for part, lane in enumerate((1 - core, core)):
            start = pl.multiple_of((there * 2 + lane) * owned + at, 16)
            amp_loads.append(pltpu.make_async_copy(
                amp_ref.at[0, pl.ds(start, piece)],
                near[step].at[REACH, pl.ds(part * piece, piece)],
                amp_sem.at[step, part]))
    int_loads = [pltpu.make_async_copy(int_ref.at[k], weights.at[pl.ds(k * depth, depth)], int_sem.at[k])
                 for k in range(slots)]
    table_loads = [pltpu.make_async_copy(cd_ref, cd_smem, table_sem.at[0]),
                   pltpu.make_async_copy(live_ref, live_smem, table_sem.at[1])]
    for load in amp_loads:
        load.start()

    barrier = pltpu.get_barrier_semaphore()
    for target in (ahead, behind, twin):
        pl.semaphore_signal(barrier, inc=1, device_id={"blk": target}, device_id_type=MESH)
    pl.semaphore_signal(barrier, inc=1, device_id={"grp": mate}, device_id_type=MESH)
    for hop in range(1, halves):
        pl.semaphore_signal(barrier, inc=1, device_id={"grp": (half + hop) % halves * 2 + core}, device_id_type=MESH)
    for load in table_loads:
        load.start()
    for step in range(steps):
        near[step][window] = jnp.zeros(near[step].shape[1:], near[step].dtype)
    pl.semaphore_wait(barrier, 3 + halves)

    def push(step, source, slot, lane, target):
        return pltpu.make_async_remote_copy(
            near[step].at[source], near[step].at[slot], amp_send.at[lane, step], amp_recv.at[slot, step],
            device_id={"blk": target}, device_id_type=MESH)

    def arrival(step, slot):
        push(step, REACH, slot, 0, twin).wait_recv()

    sent = []

    def launch(copy, when=None, first=True):
        if when is None:
            copy.start()
        else:
            pl.when(when)(copy.start)
        if first:
            sent.append(copy)

    def push_passed(step):
        if step < steps:
            launch(push(step, REACH, REACH + 2 * side, 0, behind))

    def push_kept(step, when=None, first=True):
        if 0 <= step < steps:
            launch(push(step, REACH, REACH - 2 * side, 1, ahead), when, first)

    def push_twin(step):
        if step < steps:
            launch(push(step, REACH, REACH - side, 2, twin))

    def forward(step):
        if step < steps:
            arrival(step, REACH + 2 * side)
            launch(push(step, REACH + 2 * side, REACH + side, 3, twin))
            push_twin(step + AHEAD)
            push_kept(step + PACE, paced, False)

    for step in range(steps + LEAD):
        if step < steps:
            amp_loads[2 * step].wait()
            amp_loads[2 * step + 1].wait()
            push_passed(step)
            if step < AHEAD:
                push_twin(step)
        push_kept(step - LEAD, None if step - LEAD < PACE else ~paced)
    for load in int_loads:
        load.start()

    for load in table_loads:
        load.wait()
    picks = []
    for k in range(slots):
        offset = (cd_smem[here * slots + k] - here + REACH + blocks) % blocks
        picks.append(jnp.where(k < live_smem[here], offset, window))

    pair_copies, far_copies = [], []

    def settle(step):
        hop, at, piece = chunks[step]
        pair_copies[step].wait_recv()
        total = own[step][...] + pair_in[step][...]
        if hop:
            tiles = [total[:, j:j + LANES].reshape(piece // 8, 8, LANES) for j in range(0, cols, LANES)]
            peak = functools.reduce(jnp.maximum, [jnp.max(jnp.abs(t), axis=0) for t in tiles])
            peak = jnp.maximum(peak, 1e-30)
            peak_out[step] = peak * (1 / TOP)
            for j, t in enumerate(tiles):
                code = jnp.round(t * (TOP / peak)[None]).astype(jnp.int32).astype(jnp.int16)
                far_out[step][:, j * LANES:(j + 1) * LANES] = code.reshape(piece, LANES)
            there = (half + hop) % halves * 2 + core
            pair = [pltpu.make_async_remote_copy(
                source, target, far_send.at[kind, step], far_recv.at[kind, step],
                device_id={"grp": there}, device_id_type=MESH)
                for kind, (source, target) in enumerate(((far_out[step], far_in[step]), (peak_out.at[step], peak_in.at[step])))]
            for copy in pair:
                copy.start()
            far_copies.append(pair)
        else:
            out_ref[pl.ds(at, piece)] = total

    for step in range(LOOK):
        forward(step)
    for load in int_loads:
        load.wait()
    for step in range(steps):
        piece = chunks[step][2]
        forward(step + LOOK)
        for slot in (REACH - 2 * side, REACH + side, REACH - side):
            arrival(step, slot)
        lhs = jnp.concatenate([near[step][pick] for pick in picks], axis=1)

        product = jnp.dot(lhs, weights[...], preferred_element_type=jnp.float32)
        pair_out[step][...] = product[:piece]
        own[step][...] = product[piece:]

        copy = pltpu.make_async_remote_copy(
            pair_out[step], pair_in[step], pair_send.at[step], pair_recv.at[step],
            device_id={"grp": mate}, device_id_type=MESH)
        copy.start()
        pair_copies.append(copy)
        if step >= 1:
            settle(step - 1)
    settle(steps - 1)
    for step in range(far_steps):
        hop, at, piece = chunks[step]
        for copy in far_copies[step]:
            copy.wait_recv()
        peak = peak_in[step][None]
        for j in range(0, cols, LANES):
            code = far_in[step][:, j:j + LANES].astype(jnp.int32).astype(jnp.float32)
            value = (code.reshape(piece // 8, 8, LANES) * peak).reshape(piece, LANES)
            out_ref[pl.ds(at, piece), j:j + LANES] = out_ref[pl.ds(at, piece), j:j + LANES] + value
    for copy in sent + pair_copies + [copy for pair in far_copies for copy in pair]:
        copy.wait_send()


def body(blocks, groups, amplitudes, integrals, cd_index, live_blocks, occ_energy, vir_energy):
    slots, depth, cols = integrals.shape
    rows = amplitudes.shape[1]
    owned = rows // groups
    chunks = plan(rows, groups)
    steps = len(chunks)
    far = [c for c in chunks if c[0]]
    window = 2 * REACH + 1
    f32 = [pltpu.VMEM((c[2], cols), jnp.float32) for c in chunks]
    i16 = [pltpu.VMEM((c[2], cols), jnp.int16) for c in far]
    ladder = pl.pallas_call(
        functools.partial(ladder_kernel, blocks, groups),
        out_shape=jax.ShapeDtypeStruct((owned, cols), jnp.float32),
        in_specs=[pl.BlockSpec(memory_space=pltpu.HBM)] * 4,
        out_specs=pl.BlockSpec(memory_space=pltpu.VMEM),
        scratch_shapes=[pltpu.VMEM((window + 1, 2 * c[2], depth), amplitudes.dtype) for c in chunks] + f32 * 3 + i16 * 2 + [
            pltpu.SMEM(cd_index.shape, cd_index.dtype),
            pltpu.SMEM(live_blocks.shape, live_blocks.dtype),
            pltpu.SemaphoreType.DMA((2,)),
            pltpu.VMEM((slots * depth, cols), integrals.dtype),
            pltpu.VMEM((len(far), 8, LANES), jnp.float32),
            pltpu.VMEM((len(far), 8, LANES), jnp.float32),
            pltpu.SemaphoreType.DMA((steps, 2)),
            pltpu.SemaphoreType.DMA((slots,)),
            pltpu.SemaphoreType.DMA((4, steps)),
            pltpu.SemaphoreType.DMA((window, steps)),
            pltpu.SemaphoreType.DMA((steps,)),
            pltpu.SemaphoreType.DMA((steps,)),
            pltpu.SemaphoreType.DMA((2, len(far))),
            pltpu.SemaphoreType.DMA((2, len(far))),
        ],
        compiler_params=pltpu.CompilerParams(
            collective_id=0, has_side_effects=True, vmem_limit_bytes=24 * 1024 * 1024),
    )(*[pltpu.with_memory_space_constraint(x, pltpu.HBM) for x in (cd_index, live_blocks, amplitudes, integrals)])
    denominator = vir_energy[0][None, :] - occ_energy[:, None]
    return (ladder / denominator)[None]


def solution(mesh):
    return jax.shard_map(
        functools.partial(body, mesh.shape["blk"], mesh.shape["grp"]),
        mesh=mesh,
        in_specs=(P("blk", None, "grp"), P("blk", "grp", None), P(), P(), P("grp"), P("blk", None)),
        out_specs=P("blk", "grp", None),
        check_vma=False,
    )
```

```python
import functools

import jax
import jax.numpy as jnp
from jax import lax
from jax.experimental import pallas as pl
from jax.experimental.pallas import tpu as pltpu
from jax.sharding import PartitionSpec as P

REACH = 2
FAR = (4, 4, 4, 4)
NEAR = (4, 4, 4, 4)
LEAD = 3
AHEAD = 3
LOOK = 3
PACE = 1
MESH = pl.DeviceIdType.MESH
LANES = 128
TOP = 32760.0


def plan(rows, groups):
    owned = rows // groups
    hops = groups // 2
    far = [owned * p // sum(FAR) for p in FAR]
    near = [owned * p // sum(NEAR) for p in NEAR]
    out = []
    for hop in range(1, hops + 1):
        at = 0
        for piece in (far if hop < hops else near):
            out.append((hop % hops, at, piece))
            at += piece
    return out


def ladder_kernel(blocks, groups, cd_ref, live_ref, amp_ref, int_ref, out_ref, *scratch):
    slots, depth, cols = int_ref.shape
    rows = amp_ref.shape[1]
    halves = groups // 2
    owned = rows // groups
    chunks = plan(rows, groups)
    steps = len(chunks)
    far_steps = sum(1 for c in chunks if c[0])
    window = 2 * REACH + 1
    near, own, pair_out, pair_in = (scratch[i * steps:(i + 1) * steps] for i in range(4))
    rest = scratch[4 * steps:]
    far_out, far_in = rest[:far_steps], rest[far_steps:2 * far_steps]
    (cd_smem, live_smem, table_sem, weights, peak_out, peak_in, amp_sem, int_sem, amp_send, amp_recv,
     pair_send, pair_recv, far_send, far_recv) = rest[2 * far_steps:]

    here = lax.axis_index("blk")
    me = lax.axis_index("grp")
    half, core = me // 2, me % 2
    mate = half * 2 + 1 - core
    side = 1 - 2 * (here % 2)
    twin = here + side
    ahead, behind = (here + 2 * side + blocks) % blocks, (here - 2 * side + blocks) % blocks

    low, high = here < 2, here + 2 >= blocks
    paced = ~low & ~high

    amp_loads = []
    for step, (hop, at, piece) in enumerate(chunks):
        there = (half + hop) % halves
        for part, lane in enumerate((1 - core, core)):
            start = pl.multiple_of((there * 2 + lane) * owned + at, 16)
            amp_loads.append(pltpu.make_async_copy(
                amp_ref.at[0, pl.ds(start, piece)],
                near[step].at[REACH, pl.ds(part * piece, piece)],
                amp_sem.at[step, part]))
    int_loads = [pltpu.make_async_copy(int_ref.at[k], weights.at[pl.ds(k * depth, depth)], int_sem.at[k])
                 for k in range(slots)]
    table_loads = [pltpu.make_async_copy(cd_ref, cd_smem, table_sem.at[0]),
                   pltpu.make_async_copy(live_ref, live_smem, table_sem.at[1])]
    for load in amp_loads:
        load.start()

    barrier = pltpu.get_barrier_semaphore()
    for target in (ahead, behind, twin):
        pl.semaphore_signal(barrier, inc=1, device_id={"blk": target}, device_id_type=MESH)
    pl.semaphore_signal(barrier, inc=1, device_id={"grp": mate}, device_id_type=MESH)
    for hop in range(1, halves):
        pl.semaphore_signal(barrier, inc=1, device_id={"grp": (half + hop) % halves * 2 + core}, device_id_type=MESH)
    for load in table_loads:
        load.start()
    for step in range(steps):
        near[step][window] = jnp.zeros(near[step].shape[1:], near[step].dtype)
    pl.semaphore_wait(barrier, 3 + halves)

    def push(step, source, slot, lane, target):
        return pltpu.make_async_remote_copy(
            near[step].at[source], near[step].at[slot], amp_send.at[lane, step], amp_recv.at[slot, step],
            device_id={"blk": target}, device_id_type=MESH)

    def arrival(step, slot):
        push(step, REACH, slot, 0, twin).wait_recv()

    sent = []

    def launch(copy, when=None, first=True):
        if when is None:
            copy.start()
        else:
            pl.when(when)(copy.start)
        if first:
            sent.append(copy)

    def push_passed(step):
        if step < steps:
            launch(push(step, REACH, REACH + 2 * side, 0, behind))

    def push_kept(step, when=None, first=True):
        if 0 <= step < steps:
            launch(push(step, REACH, REACH - 2 * side, 1, ahead), when, first)

    def push_twin(step):
        if step < steps:
            launch(push(step, REACH, REACH - side, 2, twin))

    def forward(step):
        if step < steps:
            arrival(step, REACH + 2 * side)
            launch(push(step, REACH + 2 * side, REACH + side, 3, twin))
            push_twin(step + AHEAD)
            push_kept(step + PACE, paced, False)

    for step in range(steps + LEAD):
        if step < steps:
            amp_loads[2 * step].wait()
            amp_loads[2 * step + 1].wait()
            push_passed(step)
            if step < AHEAD:
                push_twin(step)
        push_kept(step - LEAD, None if step - LEAD < PACE else ~paced)
    for load in int_loads:
        load.start()

    for load in table_loads:
        load.wait()
    picks = []
    for k in range(slots):
        offset = (cd_smem[here * slots + k] - here + REACH + blocks) % blocks
        picks.append(jnp.where(k < live_smem[here], offset, window))

    pair_copies, far_copies = [], []

    def settle(step):
        hop, at, piece = chunks[step]
        pair_copies[step].wait_recv()
        total = own[step][...] + pair_in[step][...]
        if hop:
            tiles = [total[:, j:j + LANES].reshape(piece // 8, 8, LANES) for j in range(0, cols, LANES)]
            peak = functools.reduce(jnp.maximum, [jnp.max(jnp.abs(t), axis=0) for t in tiles])
            peak = jnp.maximum(peak, 1e-30)
            peak_out[step] = peak * (1 / TOP)
            for j, t in enumerate(tiles):
                code = jnp.round(t * (TOP / peak)[None]).astype(jnp.int32).astype(jnp.int16)
                far_out[step][:, j * LANES:(j + 1) * LANES] = code.reshape(piece, LANES)
            there = (half + hop) % halves * 2 + core
            pair = [pltpu.make_async_remote_copy(
                source, target, far_send.at[kind, step], far_recv.at[kind, step],
                device_id={"grp": there}, device_id_type=MESH)
                for kind, (source, target) in enumerate(((far_out[step], far_in[step]), (peak_out.at[step], peak_in.at[step])))]
            for copy in pair:
                copy.start()
            far_copies.append(pair)
        else:
            out_ref[pl.ds(at, piece)] = total

    for step in range(LOOK):
        forward(step)
    for load in int_loads:
        load.wait()
    for step in range(steps):
        piece = chunks[step][2]
        forward(step + LOOK)
        for slot in (REACH - 2 * side, REACH + side, REACH - side):
            arrival(step, slot)
        lhs = jnp.concatenate([near[step][pick] for pick in picks], axis=1)

        product = jnp.dot(lhs, weights[...], preferred_element_type=jnp.float32)
        pair_out[step][...] = product[:piece]
        own[step][...] = product[piece:]

        copy = pltpu.make_async_remote_copy(
            pair_out[step], pair_in[step], pair_send.at[step], pair_recv.at[step],
            device_id={"grp": mate}, device_id_type=MESH)
        copy.start()
        pair_copies.append(copy)
        if step >= 1:
            settle(step - 1)
    settle(steps - 1)
    for step in range(far_steps):
        hop, at, piece = chunks[step]
        for copy in far_copies[step]:
            copy.wait_recv()
        peak = peak_in[step][None]
        for j in range(0, cols, LANES):
            code = far_in[step][:, j:j + LANES].astype(jnp.int32).astype(jnp.float32)
            value = (code.reshape(piece // 8, 8, LANES) * peak).reshape(piece, LANES)
            out_ref[pl.ds(at, piece), j:j + LANES] = out_ref[pl.ds(at, piece), j:j + LANES] + value
    for copy in sent + pair_copies + [copy for pair in far_copies for copy in pair]:
        copy.wait_send()


def body(blocks, groups, amplitudes, integrals, cd_index, live_blocks, occ_energy, vir_energy):
    slots, depth, cols = integrals.shape
    rows = amplitudes.shape[1]
    owned = rows // groups
    chunks = plan(rows, groups)
    steps = len(chunks)
    far = [c for c in chunks if c[0]]
    window = 2 * REACH + 1
    f32 = [pltpu.VMEM((c[2], cols), jnp.float32) for c in chunks]
    i16 = [pltpu.VMEM((c[2], cols), jnp.int16) for c in far]
    ladder = pl.pallas_call(
        functools.partial(ladder_kernel, blocks, groups),
        out_shape=jax.ShapeDtypeStruct((owned, cols), jnp.float32),
        in_specs=[pl.BlockSpec(memory_space=pltpu.HBM)] * 4,
        out_specs=pl.BlockSpec(memory_space=pltpu.VMEM),
        scratch_shapes=[pltpu.VMEM((window + 1, 2 * c[2], depth), amplitudes.dtype) for c in chunks] + f32 * 3 + i16 * 2 + [
            pltpu.SMEM(cd_index.shape, cd_index.dtype),
            pltpu.SMEM(live_blocks.shape, live_blocks.dtype),
            pltpu.SemaphoreType.DMA((2,)),
            pltpu.VMEM((slots * depth, cols), integrals.dtype),
            pltpu.VMEM((len(far), 8, LANES), jnp.float32),
            pltpu.VMEM((len(far), 8, LANES), jnp.float32),
            pltpu.SemaphoreType.DMA((steps, 2)),
            pltpu.SemaphoreType.DMA((slots,)),
            pltpu.SemaphoreType.DMA((4, steps)),
            pltpu.SemaphoreType.DMA((window, steps)),
            pltpu.SemaphoreType.DMA((steps,)),
            pltpu.SemaphoreType.DMA((steps,)),
            pltpu.SemaphoreType.DMA((2, len(far))),
            pltpu.SemaphoreType.DMA((2, len(far))),
        ],
        compiler_params=pltpu.CompilerParams(
            collective_id=0, has_side_effects=True, vmem_limit_bytes=24 * 1024 * 1024),
    )(*[pltpu.with_memory_space_constraint(x, pltpu.HBM) for x in (cd_index, live_blocks, amplitudes, integrals)])
    denominator = vir_energy[0][None, :] - occ_energy[:, None]
    return (ladder / denominator)[None]


def solution(mesh):
    return jax.shard_map(
        functools.partial(body, mesh.shape["blk"], mesh.shape["grp"]),
        mesh=mesh,
        in_specs=(P("blk", None, "grp"), P("blk", "grp", None), P(), P(), P("grp"), P("blk", None)),
        out_specs=P("blk", "grp", None),
        check_vma=False,
    )
```
